32 devices in a mesh: rows: 8 (over z, x), width: 4 (over y, core).
Axes of the slice: x: 2, y: 2, z: 4, core: 2. Of those that a mesh axis runs over, the one named last changes fastest.
Arguments:
- weight_gate: float32 [2560, 9728], P('rows', 'width'), may hold values from -0.15625 to 0.15625
- moment_gate: float32 [2560, 9728], P('rows', 'width'), may hold values from -6 to 6
- square_gate: float32 [2560, 9728], P('rows', 'width'), may hold values from 0.1 to 10
- weight_up: float32 [2560, 9728], P('rows', 'width'), may hold values from -0.15625 to 0.15625
- moment_up: float32 [2560, 9728], P('rows', 'width'), may hold values from -6 to 6
- square_up: float32 [2560, 9728], P('rows', 'width'), may hold values from 0.1 to 10
- norm_gain: float32 [2560], P('rows'), may hold values from 0.25 to 1.75
Outputs:
- ready_gate: bfloat16 [2560, 9728], P(None, 'width')
- ready_up: bfloat16 [2560, 9728], P(None, 'width')
- column_gate: float32 [9728], P('width')
- column_up: float32 [9728], P('width')
The draws below stay inside these ranges and needn't reach their ends.
All inputs are finite; a program needn't handle non-finite values.
Results may differ from the reference program's by a relative error of at most 0.0004.
Values may be sent and summed in bfloat16 or wider, within the bound.
No kernel may reach another device: no remote copies, remote signals or barrier semaphores. Data moves between devices by JAX's collectives and lax.ppermute only.
A program may use at most 128 MiB of HBM per device.

```python
import math
import jax
import jax.numpy as jnp
from jax import lax

D_MODEL = 2560
D_INNER = 9728


def with_spikes(values, rng, source, target, blocks, factor):
    def block_of(axis_at):
        return (jnp.arange(values.shape[axis_at]) // (values.shape[axis_at] // blocks)).reshape((-1,) + (1,) * (values.ndim - 1 - axis_at))

    one_side = jax.random.permutation(rng, blocks)[block_of(target)]
    second = (block_of(target) + blocks // 2) % blocks
    return jnp.where((block_of(source) == one_side) | (block_of(source) == second), factor * values, values)


def block_levels(rng, extent, pieces, smallest, top_value):
    loudness, own = 1.0, jax.random.fold_in(rng, 6)
    for dim, blocks in pieces:
        heights = jnp.exp(jax.random.uniform(jax.random.fold_in(own, dim), (blocks,), jnp.float32, smallest / len(pieces), top_value / len(pieces)))
        loudness = loudness * jnp.repeat(heights, extent[dim] // blocks).reshape([-1 if axis == dim else 1 for axis in range(len(extent))])
    return loudness


def normal_values(own_key, shape, scale, limit, split=(), held_as=jnp.bfloat16):
    array = scale * jax.random.normal(own_key, shape, jnp.float32)
    if split:
        array = array * block_levels(own_key, shape, split, -0.22, 0.18)
    return jnp.clip(array, -limit, limit).astype(held_as)


def noise_with(rng, dims, spread, most, shards, heavy, dtype=jnp.bfloat16):
    entries = spread * jax.random.normal(rng, dims, jnp.float32)
    if shards:
        entries = entries * block_levels(rng, dims, shards, -0.22, 0.18)
    return jnp.clip(with_spikes(entries, jax.random.fold_in(rng, 3), *heavy), -most, most).astype(dtype)


def setup_inputs(seed: int = 0) -> dict:
    arg_keys = jax.random.split(jax.random.key(seed), 8)
    return {
        "weight_gate": noise_with(arg_keys[0], (D_MODEL, D_INNER), D_MODEL ** -0.5, 0.15625, ((0, 8), (1, 4)), (0, 1, 8, 2.0), jnp.float32),
        "moment_gate": normal_values(arg_keys[1], (D_MODEL, D_INNER), 1.0, 6.0, ((0, 8), (1, 4)), jnp.float32),
        "square_gate": jnp.clip(jnp.exp(math.log(10.0) - 4.6051702 * jax.random.uniform(arg_keys[2], (D_MODEL, D_INNER), jnp.float32) ** block_levels(arg_keys[2], (D_MODEL, D_INNER), ((0, 8), (1, 4)), -0.2, 0.2)), 0.1, 10.0),
        "weight_up": noise_with(arg_keys[3], (D_MODEL, D_INNER), D_MODEL ** -0.5, 0.15625, ((0, 8), (1, 4)), (0, 1, 8, 2.0), jnp.float32),
        "moment_up": normal_values(arg_keys[4], (D_MODEL, D_INNER), 1.0, 6.0, ((0, 8), (1, 4)), jnp.float32),
        "square_up": jnp.clip(jnp.exp(math.log(10.0) - 4.6051702 * jax.random.uniform(arg_keys[5], (D_MODEL, D_INNER), jnp.float32) ** block_levels(arg_keys[5], (D_MODEL, D_INNER), ((0, 8), (1, 4)), -0.2, 0.2)), 0.1, 10.0),
        "norm_gain": jnp.clip(1.0 + 0.15 * jax.random.normal(arg_keys[6], (D_MODEL,), jnp.float32), 0.25, 1.75),
    }


learn_rate = 0.02
decay_rate = 0.1
tiny_value = 1e-08

def reference(weight_gate, moment_gate, square_gate, weight_up, moment_up, square_up, norm_gain):
    latest_gate = weight_gate - learn_rate * (moment_gate / (jnp.sqrt(square_gate) + tiny_value) + decay_rate * weight_gate)
    latest_up = weight_up - learn_rate * (moment_up / (jnp.sqrt(square_up) + tiny_value) + decay_rate * weight_up)
    latest_gained_gate = latest_gate * norm_gain[:, None]
    latest_gained_up = latest_up * norm_gain[:, None]
    column_gate = jnp.sqrt(lax.optimization_barrier(jnp.sum(latest_gained_gate * latest_gained_gate, axis=0)))
    ready_gate = (latest_gained_gate / column_gate).astype(jnp.bfloat16)
    column_up = jnp.sqrt(lax.optimization_barrier(jnp.sum(latest_gained_up * latest_gained_up, axis=0)))
    ready_up = (latest_gained_up / column_up).astype(jnp.bfloat16)
    return (ready_gate, ready_up, column_gate, column_up)
```

```python
import jax
import jax.numpy as jnp
from jax import lax
from jax.experimental import pallas as pl
from jax.sharding import PartitionSpec as P

learn_rate = 0.02
decay_rate = 0.1
tiny_value = 1e-08
cuts = 2


def unwritten(shape, dtype):
    return pl.pallas_call(
        lambda out_ref: None,
        out_shape=jax.ShapeDtypeStruct(shape, dtype),
        out_specs=pl.BlockSpec(memory_space=pl.ANY),
    )()


def ring_order(size):
    return list(range(0, size, 2)) + list(range(1, size, 2))[::-1]


def latest_gained(weight, moment, square, norm_gain):
    latest = weight - learn_rate * (
        moment / (jnp.sqrt(square) + tiny_value) + decay_rate * weight
    )
    return latest * norm_gain[:, None]


def total_over_rows(part, size):
    if size & (size - 1):
        return lax.psum(part, "rows")
    bit = 1
    while bit < size:
        part = part + lax.ppermute(part, "rows", [(r, r ^ bit) for r in range(size)])
        bit *= 2
    return part


def per_device(size, weight_gate, moment_gate, square_gate, weight_up, moment_up, square_up, norm_gain):
    gained = (
        latest_gained(weight_gate, moment_gate, square_gate, norm_gain),
        latest_gained(weight_up, moment_up, square_up, norm_gain),
    )
    totals = total_over_rows(jnp.stack([jnp.sum(g * g, axis=0) for g in gained]), size)
    columns = [jnp.sqrt(totals[i]) for i in range(2)]
    order = ring_order(size)
    place = {rank: at for at, rank in enumerate(order)}
    rank = lax.axis_index("rows")
    rows, width = weight_gate.shape
    ready = []
    moving = []
    for i in range(2):
        narrow = (gained[i] / columns[i]).astype(jnp.bfloat16)
        step = 1 if i == 0 else -1
        perm = [(order[at], order[(at + step) % size]) for at in range(size)]
        out = lax.dynamic_update_slice(
            unwritten((size, rows, width), jnp.bfloat16), narrow[None], (rank, 0, 0)
        )
        ready.append(out)
        piece = rows // cuts
        moving.append((step, perm, [narrow[c * piece:(c + 1) * piece] for c in range(cuts)], piece))
    for hop in range(1, size):
        for i in range(2):
            step, perm, parts, piece = moving[i]
            origin = jnp.array([order[(place[r] - step * hop) % size] for r in range(size)], jnp.int32)[rank]
            for c in range(cuts):
                parts[c] = lax.ppermute(parts[c], "rows", perm)
                ready[i] = lax.dynamic_update_slice(ready[i], parts[c][None], (origin, c * piece, 0))
    ready = [r.reshape(size * rows, width) for r in ready]
    return (ready[0], ready[1], columns[0], columns[1])


def solution(mesh):
    size = mesh.shape["rows"]
    in_specs = (
        P("rows", "width"),
        P("rows", "width"),
        P("rows", "width"),
        P("rows", "width"),
        P("rows", "width"),
        P("rows", "width"),
        P("rows"),
    )
    out_specs = (P(None, "width"), P(None, "width"), P("width"), P("width"))

    def body(*args):
        return per_device(size, *args)

    return jax.shard_map(body, mesh=mesh, in_specs=in_specs, out_specs=out_specs, check_vma=False)
```

```python
import jax
import jax.numpy as jnp
from jax import lax
from jax.experimental import pallas as pl
from jax.sharding import PartitionSpec as P


learn_rate = 0.02
decay_rate = 0.1
tiny_value = 1e-08
most_cuts = 2
reach = 4


def unwritten(shape, dtype):
    return pl.pallas_call(
        lambda out_ref: None,
        out_shape=jax.ShapeDtypeStruct(shape, dtype),
        out_specs=pl.BlockSpec(memory_space=pl.ANY),
    )()


def ring_order(size):
    return list(range(0, size, 2)) + list(range(1, size, 2))[::-1]


def latest_gained(weight, moment, square, norm_gain):
    latest = weight - learn_rate * (
        moment / (jnp.sqrt(square) + tiny_value) + decay_rate * weight
    )
    return latest * norm_gain[:, None]


def total_over_rows(part, size):
    if size & (size - 1):
        return lax.psum(part, "rows")
    bit = 1
    while bit < size:
        span = min(reach, size // bit)
        terms = [part] + [
            lax.ppermute(part, "rows", [(r, r ^ (bit * k)) for r in range(size)])
            for k in range(1, span)
        ]
        while len(terms) > 1:
            terms = [terms[k] + terms[k + 1] for k in range(0, len(terms), 2)]
        part = terms[0]
        bit *= span
    return part


def per_device(size, weight_gate, moment_gate, square_gate, weight_up, moment_up, square_up, norm_gain):
    gained = (
        latest_gained(weight_gate, moment_gate, square_gate, norm_gain),
        latest_gained(weight_up, moment_up, square_up, norm_gain),
    )
    totals = total_over_rows(jnp.stack([jnp.sum(g * g, axis=0) for g in gained]), size)
    columns = [jnp.sqrt(totals[i]) for i in range(2)]
    order = ring_order(size)
    rank = lax.axis_index("rows")
    evens = (size + 1) // 2
    place = jnp.where(rank % 2 == 0, rank // 2, size - 1 - rank // 2)
    rows, width = weight_gate.shape
    cuts = max(c for c in (most_cuts, 2, 1) if rows % (16 * c) == 0 or c == 1)
    piece = rows // cuts

    def narrow(values, i, c):
        return (values[i][c * piece:(c + 1) * piece] / columns[i]).astype(jnp.bfloat16)

    moving = [[narrow(gained, i, 0)] for i in range(2)]
    if cuts > 1:
        gained, first_gate, first_up = lax.optimization_barrier((gained, moving[0][0], moving[1][0]))
        moving = [[first_gate], [first_up]]
        for i in range(2):
            moving[i] += [narrow(gained, i, c) for c in range(1, cuts)]
    ready = [unwritten((size, rows, width), jnp.bfloat16) for _ in range(2)]
    for hop in range(size):
        for c in range(cuts):
            for i in range(2):
                step = 1 if i == 0 else -1
                if hop:
                    perm = [(order[at], order[(at + step) % size]) for at in range(size)]
                    moving[i][c] = lax.ppermute(moving[i][c], "rows", perm)
                at = (place - step * hop) % size
                origin = jnp.where(at < evens, 2 * at, 2 * (size - 1 - at) + 1)
                ready[i] = lax.dynamic_update_slice(ready[i], moving[i][c][None], (origin, c * piece, 0))
    ready = [r.reshape(size * rows, width) for r in ready]
    return (ready[0], ready[1], columns[0], columns[1])


def solution(mesh):
    size = mesh.shape["rows"]
    in_specs = (
        P("rows", "width"),
        P("rows", "width"),
        P("rows", "width"),
        P("rows", "width"),
        P("rows", "width"),
        P("rows", "width"),
        P("rows"),
    )
    out_specs = (P(None, "width"), P(None, "width"), P("width"), P("width"))

    def body(*args):
        return per_device(size, *args)

    return jax.shard_map(body, mesh=mesh, in_specs=in_specs, out_specs=out_specs, check_vma=False)
```
